256 devices in a mesh: doc: 2 (over z), seq: 16 (over y, core), head: 8 (over x).
Axes of the slice: x: 8, y: 8, z: 2, core: 2. Of those that a mesh axis runs over, the one named last changes fastest.
The devices are a block of a 8x8x16 slice.
Arguments:
- length: int32 [2], P('doc'), parts along dimension 0, may hold values from 3968 to 4096
- residual: bfloat16 [8192, 4096], P(('doc', 'seq'), 'head'), parts along dimension 0, may hold values from -6 to 6
- ssm_input: bfloat16 [8192, 4096], P(('doc', 'seq'), 'head'), parts along dimension 0, may hold values from -6 to 6
- state_in: bfloat16 [8192, 128], P(('doc', 'seq')), parts along dimension 0, may hold values from -6 to 6
- state_out: bfloat16 [8192, 128], P(('doc', 'seq')), parts along dimension 0, may hold values from -0.5 to 0.5
- step_raw: float32 [128, 4096], P(('doc', 'head'), 'seq'), parts along dimension 0, may hold values from -5 to 2
- decay_rate: float32 [64], P('head'), may hold values from 0 to 1, as said below
- ssm_gain: float32 [4096], P('head'), may hold values from 0.1 to 1.9
- out_weight: bfloat16 [4096, 4096], P('head'), may hold values from -0.09375 to 0.09375
- norm_gain: float32 [4096], replicated, may hold values from 0.1 to 1.9
- query_weight: bfloat16 [4096, 4096], P(None, 'head'), may hold values from -2 to 2
- key_weight: bfloat16 [4096, 1024], P(None, 'head'), may hold values from -3 to 3
- value_weight: bfloat16 [4096, 1024], P(None, 'head'), may hold values from -0.09375 to 0.09375
Outputs:
- layer_out: bfloat16 [8192, 4096], P(('doc', 'seq'), 'head'), parts along dimension 0
- head_out: bfloat16 [8192, 4096], P(('doc', 'seq'), 'head'), parts along dimension 0
The draws below stay inside these ranges and needn't reach their ends.
There are 2 independent parts, one for each index of `doc`. The reference program is written for one: setup_inputs(seed, part) draws one part's arguments, and reference() takes and returns one part's arrays. A program takes and returns all parts, laid end to end along the dimension named above; an argument that names none is the same for every part. Nothing has to cross between parts.
Inputs may be any that keep to these rules, and one draw needn't show every extreme that they name: The document fills positions 0 to length - 1 of the 4096; later positions are padding. `decay_rate`: positive.
All inputs are finite; a program needn't handle non-finite values.
Results may differ from the reference program's by a relative error of at most 0.028.
The reference program's roundings to bfloat16 on the way count: a program that leaves them out, or rounds other values in their place, can miss the bound.
Values may be sent and summed in bfloat16 or wider, within the bound.
No kernel may reach another device: no remote copies, remote signals or barrier semaphores. Data moves between devices by JAX's collectives and lax.ppermute only.
A program may use at most 64 MiB of HBM per device.

```python
import jax
import jax.numpy as jnp
from jax import lax

D = 4096
SSM_HEADS = 64
SSM_HDIM = 64
STATE = 128
Q_HEADS = 32
KV_HEADS = 8
HEAD_DIM = 128
TOK_DEV = 256
INNER = 4096
TOKENS = 4096


def draw_step_raw(key, part):
    blocks = TOKENS // TOK_DEV
    base = jax.random.uniform(jax.random.fold_in(key, 31), (SSM_HEADS, blocks, TOK_DEV), jnp.float32, -3.5, 1.0)
    offset = jax.random.uniform(jax.random.fold_in(key, 32), (SSM_HEADS, blocks, 1), jnp.float32, -1.5, 1.0)
    return (base + offset).reshape(SSM_HEADS, TOKENS)


def draw_decay_rate(key, part):
    order = jax.random.permutation(jax.random.fold_in(key, 21), SSM_HEADS)
    slow = order < SSM_HEADS // 2
    spread = jax.random.uniform(jax.random.fold_in(key, 22), (SSM_HEADS,), jnp.float32)
    slow_rate = jnp.exp(jnp.log(0.25 / TOKENS) + spread * jnp.log(12.0))
    fast_rate = jnp.exp(jnp.log(0.05) + spread * jnp.log(20.0))
    return jnp.where(slow, slow_rate, fast_rate)


def query_key_pair(key):
    scale = 1.6 * D ** (-0.5)
    query_part = jnp.clip(jax.random.normal(jax.random.fold_in(key, 11), (D, Q_HEADS * HEAD_DIM), jnp.float32), -6.0, 6.0) * scale
    key_part = jnp.clip(jax.random.normal(jax.random.fold_in(key, 12), (D, KV_HEADS * HEAD_DIM), jnp.float32), -6.0, 6.0) * scale
    return (query_part, key_part)


def draw_query_weight(key, part):
    return query_key_pair(key)[0].astype(jnp.bfloat16)


def draw_key_weight(key, part):
    return query_key_pair(key)[1].astype(jnp.bfloat16)


def levels(stream_key, extent, split, smallest, top_value):
    gain, own = 1.0, jax.random.fold_in(stream_key, 6)
    for dim, blocks in split:
        heights = jnp.exp(jax.random.uniform(jax.random.fold_in(own, dim), (blocks,), jnp.float32, smallest / len(split), top_value / len(split)))
        gain = gain * jnp.repeat(heights, extent[dim] // blocks).reshape([-1 if axis == dim else 1 for axis in range(len(extent))])
    return gain


def centred(rng, extent, scale, reach, shards=(), kind=jnp.bfloat16):
    drawn = scale * jax.random.normal(rng, extent, jnp.float32)
    if shards:
        drawn = drawn * levels(rng, extent, shards, -0.22, 0.18)
    return jnp.clip(drawn, -reach, reach).astype(kind)


def setup_inputs(seed: int = 0, part: int = 0) -> dict:
    key_list = jax.random.split(jax.random.key(seed), 14)
    part_keys = jax.random.split(jax.random.fold_in(key_list[13], part), 14)
    length = jax.random.randint(part_keys[0], (1,), TOKENS - TOK_DEV // 2, TOKENS + 1).astype(jnp.int32)
    residual = centred(part_keys[1], (TOKENS, D), 1.0, 6.0, ((0, 16), (1, 8)))
    ssm_input = centred(part_keys[2], (TOKENS, INNER), 1.0, 6.0, ((0, 16), (1, 8)))
    state_in = centred(part_keys[3], (TOKENS, STATE), 1.0, 6.0, ((0, 16),))
    state_out = centred(part_keys[4], (TOKENS, STATE), STATE ** -0.5, 0.5, ((0, 16),))
    step_raw = draw_step_raw(jax.random.fold_in(jax.random.fold_in(key_list[13], part), 71), part)
    decay_rate = draw_decay_rate(jax.random.fold_in(key_list[13], 71), part)
    ssm_gain = jnp.clip(1.0 + 0.18 * jax.random.normal(key_list[7], (INNER,), jnp.float32), 0.1, 1.9)
    out_weight = centred(key_list[8], (INNER, D), INNER ** -0.5, 0.09375, ((0, 8),))
    norm_gain = jnp.clip(1.0 + 0.18 * jax.random.normal(key_list[9], (D,), jnp.float32), 0.1, 1.9)
    query_weight = draw_query_weight(jax.random.fold_in(key_list[13], 71), part)
    key_weight = draw_key_weight(jax.random.fold_in(key_list[13], 71), part)
    value_weight = centred(key_list[12], (D, KV_HEADS * HEAD_DIM), D ** -0.5, 0.09375, ((1, 8),))
    return dict(length=length, residual=residual, ssm_input=ssm_input, state_in=state_in, state_out=state_out, step_raw=step_raw, decay_rate=decay_rate, ssm_gain=ssm_gain, out_weight=out_weight, norm_gain=norm_gain, query_weight=query_weight, key_weight=key_weight, value_weight=value_weight)


EPSILON = 1e-05
NEG_BIG = -1e+30
HIGHEST = lax.Precision.HIGHEST

def ssd_blocks(ssm_input, state_in, state_out, delta, decay_rate):
    blocks = TOKENS // TOK_DEV
    inputs = ssm_input.astype(jnp.float32).reshape(blocks, TOK_DEV, SSM_HEADS, SSM_HDIM)
    enter = state_in.reshape(blocks, TOK_DEV, STATE)
    leave = state_out.reshape(blocks, TOK_DEV, STATE)
    steps = delta.reshape(SSM_HEADS, blocks, TOK_DEV).transpose(1, 0, 2)
    causal = jnp.arange(TOK_DEV)[:, None] >= jnp.arange(TOK_DEV)[None, :]

    def advance(carried, inputs_now):
        block_in, enter_now, leave_now, step_now = inputs_now
        cumlog = jnp.cumsum(-decay_rate[:, None] * step_now, axis=1)
        inner = jnp.dot(leave_now, enter_now.T, preferred_element_type=jnp.float32)
        spread = cumlog[:, :, None] - cumlog[:, None, :]
        mixing = jnp.where(causal[None], jnp.exp(jnp.where(causal[None], spread, 0.0)), 0.0) * inner[None] * step_now[:, None, :]
        within = jnp.einsum('hts,shp->thp', mixing, block_in, precision=HIGHEST)
        carried_out = jnp.einsum('hpn,tn->thp', carried, leave_now.astype(jnp.float32), precision=HIGHEST)
        output = within + jnp.exp(cumlog).T[:, :, None] * carried_out
        tail = jnp.exp(cumlog[:, -1:] - cumlog) * step_now
        fresh = jnp.einsum('hs,shp,sn->hpn', tail, block_in, enter_now.astype(jnp.float32), precision=HIGHEST)
        following = jnp.exp(cumlog[:, -1])[:, None, None] * carried + fresh
        return (following, output)
    start = jnp.zeros((SSM_HEADS, SSM_HDIM, STATE), jnp.float32)
    unused, outputs = lax.scan(advance, start, (inputs, enter, leave, steps))
    return outputs.reshape(TOKENS, SSM_HEADS, SSM_HDIM)

def reference(length, residual, ssm_input, state_in, state_out, step_raw, decay_rate, ssm_gain, out_weight, norm_gain, query_weight, key_weight, value_weight):
    positions = jnp.arange(TOKENS, dtype=jnp.int32)
    live_rows = positions < length[0]
    live = live_rows.astype(jnp.float32)
    delta = live[None, :] * jax.nn.softplus(step_raw)
    ssm_out = ssd_blocks(ssm_input, state_in, state_out, delta, decay_rate) * live[:, None, None]
    mean_square = lax.optimization_barrier(jnp.mean(ssm_out * ssm_out, axis=2, keepdims=True))
    normed = (ssm_out * lax.rsqrt(mean_square + EPSILON) * ssm_gain.reshape(SSM_HEADS, SSM_HDIM)).astype(jnp.bfloat16)
    normed = normed.reshape(TOKENS, SSM_HEADS * SSM_HDIM)
    projected = jnp.dot(normed, out_weight, preferred_element_type=jnp.float32)
    layer_out = (residual.astype(jnp.float32) + projected).astype(jnp.bfloat16)
    widened = layer_out.astype(jnp.float32)
    attn_in = (widened * lax.rsqrt(lax.optimization_barrier(jnp.mean(widened * widened, axis=1, keepdims=True)) + EPSILON) * norm_gain).astype(jnp.bfloat16)
    queries = jnp.dot(attn_in, query_weight, preferred_element_type=jnp.float32).astype(jnp.bfloat16)
    keys = jnp.dot(attn_in, key_weight, preferred_element_type=jnp.float32).astype(jnp.bfloat16)
    values = jnp.dot(attn_in, value_weight, preferred_element_type=jnp.float32).astype(jnp.bfloat16)
    group_size = Q_HEADS // KV_HEADS
    query_heads = queries.reshape(TOKENS, Q_HEADS, HEAD_DIM).transpose(1, 0, 2)
    key_heads = jnp.repeat(keys.reshape(TOKENS, KV_HEADS, HEAD_DIM).transpose(1, 0, 2), group_size, axis=0)
    value_heads = jnp.repeat(values.reshape(TOKENS, KV_HEADS, HEAD_DIM).transpose(1, 0, 2), group_size, axis=0)
    allowed = (positions[None, :] <= positions[:, None]) & live_rows[None, :]

    def one_head(operands):
        query_now, key_now, value_now = operands
        scores = jnp.dot(query_now, key_now.T, preferred_element_type=jnp.float32) * HEAD_DIM ** (-0.5)
        masked = jnp.where(allowed, scores, NEG_BIG)
        best = lax.optimization_barrier(jnp.max(masked, axis=1, keepdims=True))
        weights = jnp.where(allowed, jnp.exp(masked - best), 0.0)
        total = lax.optimization_barrier(jnp.sum(weights, axis=1, keepdims=True))
        mixed = jnp.dot(weights.astype(jnp.bfloat16), value_now, preferred_element_type=jnp.float32)
        return mixed / jnp.where(live_rows[:, None], total, 1.0) * live[:, None]
    heads = lax.map(one_head, (query_heads, key_heads, value_heads))
    head_out = heads.transpose(1, 0, 2).reshape(TOKENS, Q_HEADS * HEAD_DIM).astype(jnp.bfloat16)
    return (layer_out, head_out)
```

```python
import functools

import jax
import jax.numpy as jnp
from jax import lax
from jax.experimental import pallas as pl
from jax.experimental.pallas import tpu as pltpu
from jax.sharding import Mesh
from jax.sharding import PartitionSpec as P

HEAD_DIM = 128
EPSILON = 1e-05
NEG_BIG = -1e30
SHARDS = ("row", "core")
DOC_SEQ = ("doc", "row", "core")
BF = jnp.bfloat16
F32 = jnp.float32


VMEM = pl.BlockSpec(memory_space=pltpu.VMEM)
SMEM = pl.BlockSpec(memory_space=pltpu.SMEM)


def call(kernel, outs, specs, args, flops, name, scratch=()):
    params = pltpu.CompilerParams(vmem_limit_bytes=32 * 1024 * 1024)
    many = isinstance(outs, (tuple, list))
    return pl.pallas_call(
        kernel,
        out_shape=outs,
        in_specs=list(specs),
        out_specs=tuple(VMEM for _ in outs) if many else VMEM,
        scratch_shapes=list(scratch),
        compiler_params=params,
        cost_estimate=pl.CostEstimate(flops=flops, bytes_accessed=1 << 20, transcendentals=0),
        name=name,
    )(*args)


def pieces(a, count):
    out = []
    for _ in range(count - 1):
        top = a.astype(BF)
        out.append(top)
        a = a - top.astype(F32)
    out.append(a.astype(BF))
    return out


def dot(a, b, dims=((1,), (0,))):
    return lax.dot_general(a, b, (dims, ((), ())), preferred_element_type=F32)


def split_dot(a, b, count, dims=((1,), (0,))):
    return sum(dot(part, b, dims) for part in pieces(a, count))


def dot_split(a, b, count, dims=((1,), (0,))):
    return sum(dot(a, part, dims) for part in pieces(b, count))


def iota(shape, dim):
    return lax.broadcasted_iota(jnp.int32, shape, dim)


def shard_index():
    return lax.axis_index("row") * lax.axis_size("core") + lax.axis_index("core")


def softplus(a):
    return jnp.maximum(a, 0.0) + jnp.log1p(jnp.exp(-jnp.abs(a)))


def state_kernel(length, rate, raw, x, enter, msg, cum_wide, cum_row, delta_row):
    heads, rows = raw.shape
    wide = x.shape[1]
    per = wide // heads
    positions = shard_index() * rows + iota((heads, rows), 1)
    delta = jnp.where(positions < length[0], softplus(raw[...]), 0.0)
    delta_row[...] = delta
    rate_rows = jnp.zeros((heads, rows), F32)
    rate_wide = jnp.zeros((8, wide), F32)
    for h in range(heads):
        rate_rows = jnp.where(iota((heads, rows), 0) == h, rate[h], rate_rows)
        rate_wide = jnp.where(iota((8, wide), 1) // per == h, rate[h], rate_wide)
    rate_wide = rate_wide[:1]
    after = (iota((rows, rows), 0) <= iota((rows, rows), 1)).astype(F32).astype(BF)
    cum_row[...] = split_dot(-rate_rows * delta, after, 3)
    pick = (iota((heads, wide), 1) // per == iota((heads, wide), 0)).astype(F32).astype(BF)
    delta_wide = split_dot(delta, pick, 3, ((0,), (0,)))
    before = (iota((rows, rows), 0) >= iota((rows, rows), 1)).astype(F32).astype(BF)
    cum = dot_split(before, -rate_wide * delta_wide, 3)
    cum_wide[...] = cum
    last = cum[rows - 1 : rows]
    tail = jnp.exp(last - cum) * delta_wide
    state = dot_split(enter[...], x[...].astype(F32) * tail, 3, ((0,), (0,)))
    lanes = 128
    tile = jnp.zeros((8, lanes), F32)
    for q in range(wide // lanes):
        tile = jnp.where(iota((8, lanes), 0) == q, last[:, q * lanes : (q + 1) * lanes], tile)
    count, deep = msg.shape[0], msg.shape[1]
    for d in range(count):
        msg[d, :, :wide] = state[d * deep : (d + 1) * deep]
        msg[d, :, wide:] = tile


def within_kernel(x, enter, leave, cum_wide, cum_row, delta_row, out):
    heads, rows = cum_row.shape
    per = x.shape[1] // heads
    causal = iota((rows, rows), 0) >= iota((rows, rows), 1)
    inner = dot(leave[...], enter[...], ((1,), (1,)))
    inner = jnp.where(causal, inner, 0.0)
    for h in range(heads):
        spread = cum_wide[:, h * per : h * per + 1] - cum_row[h : h + 1, :]
        mixing = jnp.exp(jnp.where(causal, spread, NEG_BIG)) * inner * delta_row[h : h + 1, :]
        out[:, h * per : (h + 1) * per] = split_dot(mixing, x[:, h * per : (h + 1) * per], 2)


def prefix_kernel(got, out):
    count, deep, wide = out.shape
    lanes = 128
    state = jnp.zeros((deep, wide), F32)
    for j in range(count):
        out[j] = state
        keep = jnp.exp(got[j, :, wide:])
        keep = jnp.concatenate(
            [jnp.broadcast_to(keep[q : q + 1], (deep, lanes)) for q in range(wide // lanes)], axis=1
        )
        state = state * keep + got[j, :, :wide]


def norm_kernel(per, length, state, leave, cum_wide, within, gain, weight, normed, first):
    rows, wide = cum_wide.shape
    carried = dot_split(leave[...], state[...], 3)
    live = (shard_index() * rows + iota((rows, 1), 0)) < length[0]
    y = within[...] + jnp.exp(cum_wide[...]) * carried
    y = jnp.where(live, y, 0.0)
    same = (iota((wide, wide), 0) // per == iota((wide, wide), 1) // per).astype(F32).astype(BF)
    mean = split_dot(y * y, same, 3) * (1.0 / per)
    value = (y * lax.rsqrt(mean + EPSILON) * gain[...]).astype(BF)
    normed[...] = value
    parts = lax.axis_size("head")
    width = first.shape[1]
    at = lax.rem(lax.axis_index("head") + parts // 2, parts)
    piece = weight[:, pl.ds(pl.multiple_of(at * width, width), width)]
    first[...] = dot(value, piece).astype(BF)


def project_kernel(offsets, normed, weight, out):
    parts = lax.axis_size("head")
    width = out.shape[2]
    value = normed[...]
    for i, k in enumerate(offsets):
        at = lax.rem(lax.axis_index("head") + (k + parts), parts)
        piece = weight[:, pl.ds(pl.multiple_of(at * width, width), width)]
        out[i] = dot(value, piece)


def qkv_kernel(order, blocks, gain, wq, wk, wv, *refs):
    parts_in, (q_out, kv_out) = refs[:-2], refs[-2:]
    parts = lax.axis_size("head")
    rows, width = q_out.shape[0], parts_in[0].shape[1]
    total = parts * width
    half = rows // 2

    def block(k, part):
        return jnp.concatenate([parts_in[i][...] for i in order[part][k]], axis=0)

    for part in range(2):
        square = jnp.zeros((half, 1), F32)
        for k in blocks:
            value = block(k, part).astype(F32)
            square = square + jnp.sum(value * value, axis=1, keepdims=True)
        scale = lax.rsqrt(square * (1.0 / total) + EPSILON)
        q = jnp.zeros((half, q_out.shape[1]), F32)
        keys = jnp.zeros((half, wk.shape[1]), F32)
        values = jnp.zeros((half, wv.shape[1]), F32)
        for k in blocks:
            at = lax.rem(lax.axis_index("head") + (k + parts), parts)
            span = pl.ds(pl.multiple_of(at * width, width), width)
            scaled = (block(k, part).astype(F32) * scale * gain[pl.ds(at, 1), :]).astype(BF)
            q = q + dot(scaled, wq[span, :])
            keys = keys + dot(scaled, wk[span, :])
            values = values + dot(scaled, wv[span, :])
        here = slice(part * half, (part + 1) * half)
        q_out[here, :] = q.astype(BF)
        kv_out[here, :] = jnp.concatenate([keys, values], axis=1).astype(BF)


def attention_kernel(groups, length, q, *refs):
    held, out, best, total, accum = refs[:-4], refs[-4], refs[-3], refs[-2], refs[-1]
    rows = q.shape[0]
    heads = q.shape[1] // HEAD_DIM
    scale = HEAD_DIM**-0.5
    row, core = lax.axis_index("row"), lax.axis_index("core")
    count = lax.axis_size("row")
    start = shard_index() * rows

    def update(h, parts, allowed, first):
        query = q[:, h * HEAD_DIM : (h + 1) * HEAD_DIM]
        scores = [dot(query, kv[:, :HEAD_DIM], ((1,), (1,))) for kv in parts]
        if allowed is not None:
            scores = [jnp.where(allowed, s, NEG_BIG) for s in scores]
        new = functools.reduce(
            jnp.maximum, [jnp.max(s, axis=1, keepdims=True) for s in scores]
        )
        if not first:
            old = best[h][:, :1]
            new = jnp.maximum(old, new)
            keep = jnp.exp((old - new) * scale)
        weights = [jnp.exp((s - new) * scale) for s in scores]
        if allowed is not None:
            weights = [jnp.where(allowed, w, 0.0) for w in weights]
        sums = sum(jnp.sum(w, axis=1, keepdims=True) for w in weights)
        mixed = sum(dot(w.astype(BF), kv[:, HEAD_DIM:]) for w, kv in zip(weights, parts))
        if not first:
            sums = sums + total[h][:, :1] * keep
            mixed = mixed + accum[h] * keep
        best[h] = jnp.broadcast_to(new, best.shape[1:])
        total[h] = jnp.broadcast_to(sums, total.shape[1:])
        accum[h] = mixed

    query_at = start + iota((rows, rows), 0)
    key_at = start + iota((rows, rows), 1)
    allowed = (key_at <= query_at) & (key_at < length[0])
    for h in range(heads):
        update(h, [held[0]], allowed, True)

    @pl.when(core > 0)
    def _():
        for h in range(heads):
            update(h, [held[1]], None, False)

    for offset, members in groups:
        source = lax.rem(row + (count - offset), count)

        @pl.when(source < row)
        def _(members=members):
            for h in range(heads):
                update(h, [held[i] for i in members], None, False)

    live = (start + iota((rows, 1), 0)) < length[0]
    for h in range(heads):
        value = accum[h] / jnp.where(live, total[h][:, :1], 1.0)
        out[:, h * HEAD_DIM : (h + 1) * HEAD_DIM] = jnp.where(live, value, 0.0).astype(BF)


def shift(x, axis, by):
    count = lax.axis_size(axis)
    return lax.ppermute(x, axis, [(i, (i + by) % count) for i in range(count)])


def swap(x):
    return shift(x, "core", 1)


def body(
    length,
    residual,
    ssm_input,
    state_in,
    state_out,
    step_raw,
    decay_rate,
    ssm_gain,
    out_weight,
    norm_gain,
    query_weight,
    key_weight,
    value_weight,
):
    rows, own = residual.shape
    heads = decay_rate.shape[0]
    wide = ssm_input.shape[1]
    deep = state_in.shape[1]
    parts = lax.axis_size("head")
    shards = lax.axis_size("row") * lax.axis_size("core")
    sds = jax.ShapeDtypeStruct

    msg, cum_wide, cum_row, delta_row = call(
        state_kernel,
        (
            sds((shards, deep // shards, wide + 128), F32),
            sds((rows, wide), F32),
            sds((heads, rows), F32),
            sds((heads, rows), F32),
        ),
        (SMEM, SMEM, VMEM, VMEM, VMEM),
        (length, decay_rate, step_raw, ssm_input, state_in),
        10**9,
        "state",
    )
    got = lax.all_to_all(msg, SHARDS, split_axis=0, concat_axis=0, tiled=True)
    within = call(
        within_kernel,
        sds((rows, wide), F32),
        (VMEM,) * 6,
        (ssm_input, state_in, state_out, cum_wide, cum_row, delta_row),
        10**9,
        "within",
    )
    before = call(
        prefix_kernel, sds((shards, deep // shards, wide), F32), (VMEM,), (got,), 10**7, "prefix"
    )
    state = lax.all_to_all(before, SHARDS, split_axis=0, concat_axis=0, tiled=True)
    state = state.reshape(deep, wide)
    normed, first = call(
        functools.partial(norm_kernel, wide // heads),
        (sds((rows, wide), BF), sds((rows, own), BF)),
        (SMEM,) + (VMEM,) * 6,
        (length, state, state_out, cum_wide, within, ssm_gain.reshape(1, wide), out_weight),
        10**9,
        "norm",
    )
    offsets = (3, -3, 2, -2, 1, -1, 0)
    products = call(
        functools.partial(project_kernel, offsets),
        sds((len(offsets), rows, own), F32),
        (VMEM, VMEM),
        (normed, out_weight),
        10**9,
        "project",
    )
    half = rows // 2
    side = own // 2

    def product(k, part):
        return products[offsets.index(k), part * half : (part + 1) * half]

    def add_left(a, got):
        return jnp.concatenate([a[:, :side] + got.astype(F32), a[:, side:]], axis=1).astype(BF)

    def add_right(a, got):
        return jnp.concatenate([a[:, :side], a[:, side:] + got.astype(F32)], axis=1).astype(BF)

    up = [first[p * half : (p + 1) * half, :side] for p in range(2)]
    down = [first[p * half : (p + 1) * half, side:] for p in range(2)]
    for step in range(parts // 2):
        up = [shift(u, "head", 1) for u in up]
        down = [shift(d, "head", -1) for d in down]
        k = parts // 2 - 1 - step
        if k == 0:
            break
        if step == 0:
            up = [add_left(product(k, p), up[p]) for p in range(2)]
            down = [add_right(product(-k, p), down[p]) for p in range(2)]
        else:
            up = [(product(k, p) + up[p].astype(F32)).astype(BF) for p in range(2)]
            down = [(product(-k, p) + down[p].astype(F32)).astype(BF) for p in range(2)]
    layer = []
    for p in range(2):
        kept = residual[p * half : (p + 1) * half].astype(F32)
        summed = product(0, p) + (up[p].astype(F32) + down[p].astype(F32))
        layer.append((kept + summed).astype(BF))
    layer_out = jnp.concatenate(layer, axis=0)

    operands = []
    order = [{}, {}]

    def note(part, k, *arrays):
        order[part][k] = tuple(range(len(operands), len(operands) + len(arrays)))
        operands.extend(arrays)

    for p in range(2):
        note(p, 0, layer[p])
    up, down = list(layer), list(layer)
    for step in range(parts // 2):
        if step == parts // 2 - 1:
            up = [u[: half // 2] for u in up]
            down = [d[half // 2 :] for d in down]
        up = [shift(u, "head", 1) for u in up]
        down = [shift(d, "head", -1) for d in down]
        for p in range(2):
            if step == parts // 2 - 1:
                note(p, parts // 2, up[p], down[p])
            else:
                note(p, -(step + 1), up[p])
                note(p, step + 1, down[p])
    queries, kv = call(
        functools.partial(qkv_kernel, order, (0, 1, -1, 2, -2, 3, -3, 4)),
        (sds((rows, query_weight.shape[1]), BF), sds((rows, 2 * key_weight.shape[1]), BF)),
        (VMEM,) * (4 + len(operands)),
        (norm_gain.reshape(parts, own), query_weight, key_weight, value_weight, *operands),
        2 * 10**9,
        "qkv",
    )

    held = [kv, swap(kv)]
    groups = []
    up = down = kv
    count = lax.axis_size("row")
    for step in range(count // 2):
        if step == count // 2 - 1:
            up, down = up[:half], down[half:]
        up, down = shift(up, "row", 1), shift(down, "row", -1)
        at = len(held)
        held += [up, swap(up), down, swap(down)]
        if step == count // 2 - 1:
            groups.append((step + 1, tuple(range(at, at + 4))))
        else:
            groups.append((step + 1, (at, at + 1)))
            groups.append((count - step - 1, (at + 2, at + 3)))
    q_heads = query_weight.shape[1] // HEAD_DIM
    head_out = call(
        functools.partial(attention_kernel, groups),
        sds(queries.shape, BF),
        (SMEM,) + (VMEM,) * (1 + len(held)),
        (length, queries, *held),
        2 * 10**9,
        "attention",
        [pltpu.VMEM((q_heads, rows, 128), F32) for _ in range(3)],
    )
    return (layer_out, head_out)


def solution(mesh):
    cores = 2
    torus = Mesh(
        mesh.devices.reshape(
            mesh.shape["doc"], mesh.shape["seq"] // cores, cores, mesh.shape["head"]
        ),
        ("doc", "row", "core", "head"),
    )
    in_specs = (
        P("doc"),
        P(DOC_SEQ, "head"),
        P(DOC_SEQ, "head"),
        P(DOC_SEQ, None),
        P(DOC_SEQ, None),
        P(("doc", "head"), SHARDS),
        P("head"),
        P("head"),
        P("head", None),
        P(),
        P(None, "head"),
        P(None, "head"),
        P(None, "head"),
    )
    out_specs = (P(DOC_SEQ, "head"), P(DOC_SEQ, "head"))
    return jax.shard_map(body, mesh=torus, in_specs=in_specs, out_specs=out_specs, check_vma=False)
```
